32 devices in a mesh: dp: 2 (over x), row: 4 (over y, core), col: 4 (over z).
Axes of the slice: x: 2, y: 2, z: 4, core: 2. Of those that a mesh axis runs over, the one named last changes fastest.
Arguments:
- layer_in: bfloat16 [4096, 1536], P(('dp', 'col'), 'row'), may hold values from -6 to 6
- cotangent: bfloat16 [4096, 1536], P(('dp', 'col'), 'row'), may hold values from -6 to 6
- doc_ids: int32 [2, 2048], P('dp'), may hold values from 0 to 2, never falling along the last dimension, each value on 1 to 1024 neighbouring positions
- pic_starts: int32 [2, 2], P('dp'), may hold values from 0 to 1792, as said below
- gain_one: float32 [1536], P('row'), may hold values from 0.25 to 1.75
- w_query: bfloat16 [1536, 1536], P('row', 'col'), may hold values from -0.15625 to 0.15625
- b_query: float32 [1536], P('col'), may hold values from -3 to 3
- w_key: bfloat16 [1536, 256], P('row'), may hold values from -0.15625 to 0.15625
- b_key: float32 [256], replicated, may hold values from -3 to 3
- w_value: bfloat16 [1536, 256], P('row'), may hold values from -0.15625 to 0.15625
- b_value: float32 [256], replicated, may hold values from -0.6 to 0.6
- w_out: bfloat16 [1536, 1536], P('col', 'row'), may hold values from -1.5 to 1.5
- gain_two: float32 [1536], P('row'), may hold values from 0.25 to 1.75
- w_gate: bfloat16 [1536, 8960], P('row', 'col'), may hold values from -0.15625 to 0.15625
- w_up: bfloat16 [1536, 8960], P('row', 'col'), may hold values from -0.15625 to 0.15625
- w_down: bfloat16 [8960, 1536], P('col', 'row'), may hold values from -0.0625 to 0.0625
Outputs:
- layer_out: bfloat16 [4096, 1536], P(('dp', 'col'), 'row')
- grad_input: float32 [4096, 1536], P(('dp', 'col'), 'row')
- grad_gain_one: float32 [1536], P('row')
- grad_w_query: float32 [1536, 1536], P('row', 'col')
- grad_b_query: float32 [1536], P('col')
- grad_w_key: float32 [1536, 256], P('row')
- grad_b_key: float32 [256], replicated
- grad_w_value: float32 [1536, 256], P('row')
- grad_b_value: float32 [256], replicated
- grad_w_out: float32 [1536, 1536], P('col', 'row')
- grad_gain_two: float32 [1536], P('row')
- grad_w_gate: float32 [1536, 8960], P('row', 'col')
- grad_w_up: float32 [1536, 8960], P('row', 'col')
- grad_w_down: float32 [8960, 1536], P('col', 'row')
The draws below stay inside these ranges and needn't reach their ends.
Inputs may be any that keep to these rules, and one draw needn't show every extreme that they name: `doc_ids`: in each row document numbers never fall; each of the 3 documents has 1 to 1024 tokens, one exactly 1024. `pic_starts`: each row lists 2 starts in rising order; start i lies between i * 1024 and (i + 1) * 1024 - 256, so pieces never intersect; a piece may reach over a document's end.
All inputs are finite; a program needn't handle non-finite values.
Results may differ from the reference program's by a relative error of at most 0.018.
Values may be sent and summed in bfloat16 or wider, within the bound.
A program may use at most 256 MiB of HBM per device.

```python
import math
import jax
import jax.numpy as jnp
import numpy as np
from jax import lax

D = 1536
FF = 8960
HEADS = 12
KV = 2
HD = 128
PIECE = 256
PACK = 2048
TOKENS = 4096
QH = 1536
KVW = 256
DOC_MAX = 1024
DOCS = 3
PICS = 2
N_DP = 2


def draw_pic_starts(key, part):
    region = PACK // PICS
    offsets = jax.random.randint(key, (N_DP, PICS), 0, region - PIECE + 1, dtype=jnp.int32)
    return (jnp.arange(PICS, dtype=jnp.int32)[None, :] * region + offsets).astype(jnp.int32)


def levels(rng, dims, cuts, low, largest):
    gain, own = 1.0, jax.random.fold_in(rng, 6)
    for position, parts in cuts:
        heights = jnp.exp(jax.random.uniform(jax.random.fold_in(own, position), (parts,), jnp.float32, low / len(cuts), largest / len(cuts)))
        gain = gain * jnp.repeat(heights, dims[position] // parts).reshape([-1 if axis == position else 1 for axis in range(len(dims))])
    return gain


def split_up(amount, total, most, skew):
    weights = [(1 << 20) // math.isqrt(standing ** skew) + 1 for standing in range(2, amount + 1)]
    spare, given = total - most - (amount - 1), [1] * (amount - 1)
    while spare > 0:
        free = [i for i in range(amount - 1) if given[i] < most]
        mass, remaining = sum([weights[i] for i in free]), spare
        for i in free:
            extra = min(most - given[i], max(1, remaining * weights[i] // mass), spare)
            given[i] = given[i] + extra
            spare = spare - extra
    return np.array([most] + given)


def ragged(stream_key, number_of, total, bound, lean):
    if number_of == 2:
        one = jax.random.randint(stream_key, (), max(1, total - bound), min(bound, total - 1) + 1)
        return jnp.stack([one, total - one])
    tallies = jnp.asarray(split_up(number_of, total, bound, lean), jnp.int32)
    twos = (number_of - 1) // 2
    giver, sink = tallies[1:1 + 2 * twos:2], tallies[2:2 + 2 * twos:2]
    slack = jnp.minimum(giver - 1, bound - sink)
    passed = jax.random.randint(jax.random.fold_in(stream_key, 1), (twos,), 0, 1 << 20) % (slack + 1)
    tallies = tallies.at[1:1 + 2 * twos:2].set(giver - passed).at[2:2 + 2 * twos:2].set(sink + passed)
    return tallies[jax.random.permutation(jax.random.fold_in(stream_key, 2), number_of)]


def centred(stream_key, shape, deviation, most, cuts=(), kind=jnp.bfloat16):
    factor_of = levels(stream_key, shape, cuts, -0.22, 0.18) if cuts else 1.0
    entries = jax.random.normal(stream_key, shape, jnp.float32) * deviation * factor_of
    return jnp.minimum(jnp.maximum(entries, -most), most).astype(kind)


def setup_inputs(seed: int = 0) -> dict:
    key_of = jax.random.split(jax.random.key(seed), 17)
    return {
        "layer_in": centred(key_of[0], (TOKENS, D), 1.0, 6.0, ((0, 8), (1, 4))),
        "cotangent": centred(key_of[1], (TOKENS, D), 1.0, 6.0, ((0, 8), (1, 4))),
        "doc_ids": jax.vmap(lambda own: jnp.searchsorted(jnp.cumsum(ragged(own, DOCS, PACK, DOC_MAX, 0)), jnp.arange(PACK), side="right"))(jax.random.split(key_of[2], N_DP)).reshape((N_DP, PACK)).astype(jnp.int32),
        "pic_starts": draw_pic_starts(jax.random.fold_in(key_of[16], 71), 0),
        "gain_one": jnp.clip(1.0 + 0.15 * jax.random.normal(key_of[4], (D,), jnp.float32), 0.25, 1.75),
        "w_query": centred(key_of[5], (D, QH), D ** -0.5, 0.15625, ((0, 4), (1, 4))),
        "b_query": centred(key_of[6], (QH,), 0.5, 3.0, ((0, 4),), jnp.float32),
        "w_key": centred(key_of[7], (D, KVW), D ** -0.5, 0.15625, ((0, 4),)),
        "b_key": centred(key_of[8], (KVW,), 0.5, 3.0, (), jnp.float32),
        "w_value": centred(key_of[9], (D, KVW), D ** -0.5, 0.15625, ((0, 4),)),
        "b_value": centred(key_of[10], (KVW,), 0.1, 0.6, (), jnp.float32),
        "w_out": centred(key_of[11], (QH, D), 16 ** -0.5, 1.5, ((0, 4), (1, 4))),
        "gain_two": jnp.clip(1.0 + 0.15 * jax.random.normal(key_of[12], (D,), jnp.float32), 0.25, 1.75),
        "w_gate": centred(key_of[13], (D, FF), D ** -0.5, 0.15625, ((0, 4), (1, 4))),
        "w_up": centred(key_of[14], (D, FF), D ** -0.5, 0.15625, ((0, 4), (1, 4))),
        "w_down": centred(key_of[15], (FF, D), FF ** -0.5, 0.0625, ((0, 4), (1, 4))),
    }


EPS = 1e-06
THETA = 10000.0
MASKED = -1e+30

@jax.custom_vjp
def low(v):
    return lax.optimization_barrier(v.astype(jnp.bfloat16)).astype(jnp.float32)

@jax.custom_vjp
def low_back(v):
    return v

def low_keep(v):
    return (low(v), None)

def low_pass(kept, grad):
    return (grad,)

def back_keep(v):
    return (v, None)

def back_low(kept, grad):
    return (low(grad),)
low.defvjp(low_keep, low_pass)
low_back.defvjp(back_keep, back_low)

def matmul(left, right):
    return jnp.dot(left, right, precision=lax.Precision.HIGHEST)

def positions(doc_row):
    places = jnp.arange(doc_row.shape[0], dtype=jnp.int32)
    before = jnp.concatenate([doc_row[:1] - 1, doc_row[:-1]])
    begins = jnp.where(doc_row != before, places, 0).astype(jnp.int32)
    return places - lax.cummax(begins, axis=0)

def picture_ids(start_list, places):
    inside = (places[None, :] >= start_list[:, None]) & (places[None, :] < start_list[:, None] + PIECE)
    labels = jnp.arange(1, start_list.shape[0] + 1, dtype=jnp.int32)
    return lax.optimization_barrier(jnp.sum(jnp.where(inside, labels[:, None], 0), axis=0, dtype=jnp.int32)) - 1

def mask_table(doc_query, pic_query, place_query, doc_key, pic_key, place_key):
    same_doc = doc_query[:, None] == doc_key[None, :]
    causal = place_key[None, :] <= place_query[:, None]
    same_pic = (pic_query[:, None] == pic_key[None, :]) & (pic_query[:, None] >= 0)
    return same_doc & (causal | same_pic)

def rope_tables(where_in_doc):
    half_dim = HD // 2
    frequency = THETA ** (-2.0 * jnp.arange(half_dim, dtype=jnp.float32) / HD)
    angles = where_in_doc.astype(jnp.float32)[:, None] * frequency[None, :]
    angles = jnp.concatenate([angles, angles], axis=1)
    return (jnp.cos(angles), jnp.sin(angles))

def rotary(values, cosine_table, sine_table):
    half_dim = values.shape[-1] // 2
    turned = jnp.concatenate([-values[..., half_dim:], values[..., :half_dim]], axis=-1)
    return values * cosine_table[:, None, :] + turned * sine_table[:, None, :]

def attend(q_rot, k_rot, value_low, allowed):
    score_scale = HD ** (-0.5)

    def one_head(pieces_in):
        query_head, key_head, value_head = pieces_in
        scores = low_back(matmul(query_head, key_head.T) * score_scale)
        scores = jnp.where(allowed, scores, MASKED)
        row_peak = lax.optimization_barrier(jnp.max(scores, axis=-1, keepdims=True))
        exponent = jnp.exp(scores - row_peak)
        weights = low(exponent / lax.optimization_barrier(jnp.sum(exponent, axis=-1, keepdims=True)))
        return matmul(weights, value_head)
    group_size = HEADS // KV
    key_heads = jnp.repeat(jnp.transpose(k_rot, (1, 0, 2)), group_size, axis=0)
    value_heads = jnp.repeat(jnp.transpose(value_low, (1, 0, 2)), group_size, axis=0)
    mixed_rows = lax.map(jax.checkpoint(one_head), (jnp.transpose(q_rot, (1, 0, 2)), key_heads, value_heads))
    return jnp.transpose(mixed_rows, (1, 0, 2))

def block_layer(state_rows, params, cosine_table, sine_table, allowed):
    gain_one, w_query, b_query, w_key, b_key, w_value, b_value, w_out, gain_two, w_gate, w_up, w_down = params
    row_count = state_rows.shape[0]
    inverse_one = lax.rsqrt(lax.optimization_barrier(jnp.mean(state_rows * state_rows, axis=-1, keepdims=True)) + EPS)
    normed_one = low(state_rows * inverse_one * gain_one)
    query = low_back(matmul(normed_one, w_query) + b_query)
    key_pre = low_back(matmul(normed_one, w_key) + b_key)
    value_low = low(low_back(matmul(normed_one, w_value) + b_value))
    q_rot = low(rotary(query.reshape(row_count, HEADS, HD), cosine_table, sine_table))
    k_rot = low(rotary(key_pre.reshape(row_count, KV, HD), cosine_table, sine_table))
    mixed_rows = attend(q_rot, k_rot, value_low.reshape(row_count, KV, HD), allowed)
    heads_out = low(low_back(mixed_rows.reshape(row_count, HEADS * HD)))
    hidden_state = state_rows + low_back(matmul(heads_out, w_out))
    inverse_two = lax.rsqrt(lax.optimization_barrier(jnp.mean(hidden_state * hidden_state, axis=-1, keepdims=True)) + EPS)
    normed_two = low(hidden_state * inverse_two * gain_two)
    gate = low_back(matmul(normed_two, w_gate))
    up_rows = low_back(matmul(normed_two, w_up))
    inner = low(jax.nn.silu(gate) * up_rows)
    return hidden_state + matmul(inner, w_down)

def reference(layer_in, cotangent, doc_ids, pic_starts, gain_one, w_query, b_query, w_key, b_key, w_value, b_value, w_out, gain_two, w_gate, w_up, w_down):
    weights = tuple((weight_in.astype(jnp.float32) for weight_in in (gain_one, w_query, b_query, w_key, b_key, w_value, b_value, w_out, gain_two, w_gate, w_up, w_down)))
    totals = tuple((jnp.zeros_like(weight_in) for weight_in in weights))
    outputs = []
    input_grads = []
    places = jnp.arange(PACK, dtype=jnp.int32)
    for pack_index in range(N_DP):
        first_row = pack_index * PACK
        state_rows = layer_in[first_row:first_row + PACK].astype(jnp.float32)
        seed_grad = cotangent[first_row:first_row + PACK].astype(jnp.float32)
        doc_row = doc_ids[pack_index]
        pic_ids = picture_ids(pic_starts[pack_index], places)
        cosine_table, sine_table = rope_tables(positions(doc_row))
        allowed = mask_table(doc_row, pic_ids, places, doc_row, pic_ids, places)

        def run_layer(state_in, *params):
            return block_layer(state_in, params, cosine_table, sine_table, allowed)
        result, pullback = jax.vjp(run_layer, state_rows, *weights)
        gradients = pullback(seed_grad)
        outputs.append(result.astype(jnp.bfloat16))
        input_grads.append(gradients[0])
        totals = tuple((total_in + grad_in for total_in, grad_in in zip(totals, gradients[1:])))
    layer_out = jnp.concatenate(outputs, axis=0)
    grad_input = jnp.concatenate(input_grads, axis=0)
    return (layer_out, grad_input, totals[0], totals[1], totals[2], totals[3], totals[4], totals[5], totals[6], totals[7], totals[8], totals[9], totals[10], totals[11])
```

```python
import jax
import jax.numpy as jnp
from jax import lax
from jax.sharding import PartitionSpec as P

D = 1536
HEADS = 12
KV = 2
HD = 128
PIECE = 256


EPS = 1e-06
THETA = 10000.0
MASKED = -1e30


BF = jnp.bfloat16
F32 = jnp.float32


def matmul(left, right):
    return jnp.dot(left, right, preferred_element_type=F32)


def contract_rows(left, right):
    return lax.dot_general(left, right, (((0,), (0,)), ((), ())), preferred_element_type=F32)


def contract_cols(left, right):
    return lax.dot_general(left, right, (((1,), (1,)), ((), ())), preferred_element_type=F32)


def rotary(values, cosine_table, sine_table):
    half_dim = values.shape[-1] // 2
    turned = jnp.concatenate([-values[..., half_dim:], values[..., :half_dim]], axis=-1)
    return values * cosine_table[:, None, :] + turned * sine_table[:, None, :]


def rotary_back(grads_in, cosine_table, sine_table):
    half_dim = grads_in.shape[-1] // 2
    scaled = grads_in * sine_table[:, None, :]
    turned = jnp.concatenate([scaled[..., half_dim:], -scaled[..., :half_dim]], axis=-1)
    return grads_in * cosine_table[:, None, :] + turned


def token_gather(values):
    return lax.all_gather(values, "col", axis=0, tiled=True)


def token_reduce(values):
    return lax.psum_scatter(values.astype(BF), "col", scatter_dimension=0, tiled=True).astype(F32)


def exchange(values, axis, step):
    size = lax.axis_size(axis)
    return lax.ppermute(values, axis, [(i, i ^ step) for i in range(size)])


def pack_total(values):
    low = values.astype(BF)
    if lax.axis_size("dp") == 2:
        return low.astype(F32) + exchange(low, "dp", 1).astype(F32)
    return lax.psum(low, "dp").astype(F32)


def weight_total(term_fn, axis):
    away = term_fn(1).astype(BF)
    here = term_fn(0) + exchange(away, "row", 1).astype(F32)
    half = here.shape[axis] // 2
    mine = lax.slice_in_dim(here, 0, half, axis=axis)
    other = lax.slice_in_dim(here, half, 2 * half, axis=axis).astype(BF)
    return mine + exchange(other, "row", 2).astype(F32)


def body(
    layer_in,
    cotangent,
    doc_ids,
    pic_starts,
    gain_one,
    w_query,
    b_query,
    w_key,
    b_key,
    w_value,
    b_value,
    w_out,
    gain_two,
    w_gate,
    w_up,
    w_down,
):
    row_devices = lax.axis_size("row")
    col_devices = lax.axis_size("col")
    row_place = lax.axis_index("row")
    col_place = lax.axis_index("col")
    packed = doc_ids.shape[1]
    chunk = layer_in.shape[0]
    owned = chunk // row_devices
    query_count = owned * col_devices
    width = layer_in.shape[1]
    heads_here = HEADS // col_devices
    head_width = heads_here * HD
    group_size = HEADS // KV
    shared_head = col_place * heads_here // group_size
    score_scale = HD ** (-0.5)

    doc_row = doc_ids[0]
    starts = pic_starts[0]

    def row_places(row):
        return (
            jnp.arange(col_devices, dtype=jnp.int32)[:, None] * chunk
            + row * owned
            + jnp.arange(owned, dtype=jnp.int32)[None, :]
        ).reshape(-1)

    places = row_places(row_place)
    key_places = jnp.concatenate([row_places(row) for row in range(row_devices)])
    doc_grid = doc_row.reshape(col_devices, row_devices, owned)
    key_docs = doc_grid.transpose(1, 0, 2).reshape(packed)
    docs = lax.dynamic_slice_in_dim(key_docs, row_place * query_count, query_count, 0)

    def picture_of(where):
        inside = (where[None, :] >= starts[:, None]) & (where[None, :] < starts[:, None] + PIECE)
        labels = jnp.arange(1, starts.shape[0] + 1, dtype=jnp.int32)
        return jnp.sum(jnp.where(inside, labels[:, None], 0), axis=0, dtype=jnp.int32) - 1

    pics = picture_of(places)
    key_pics = picture_of(key_places)
    doc_begin = jnp.sum((doc_row[None, :] < docs[:, None]).astype(jnp.int32), axis=1)
    where_in_doc = places - doc_begin
    half_dim = HD // 2
    frequency = THETA ** (-2.0 * jnp.arange(half_dim, dtype=F32) / HD)
    angles = where_in_doc.astype(F32)[:, None] * frequency[None, :]
    angles = jnp.concatenate([angles, angles], axis=1)
    cosine, sine = jnp.cos(angles), jnp.sin(angles)
    allowed = (docs[:, None] == key_docs[None, :]) & (
        (key_places[None, :] <= places[:, None])
        | ((pics[:, None] == key_pics[None, :]) & (pics[:, None] >= 0))
    )

    def kv_cols(weight):
        return lax.dynamic_slice_in_dim(weight, shared_head * HD, HD, 1)

    qkv_own = jnp.concatenate([w_query, kv_cols(w_key), kv_cols(w_value)], axis=1)
    w_qkv = lax.all_gather(qkv_own, "row", axis=0, tiled=True)
    wo_full = lax.all_gather(w_out, "row", axis=1, tiled=True)
    gate_full = lax.all_gather(w_gate, "row", axis=0, tiled=True)
    up_full = lax.all_gather(w_up, "row", axis=0, tiled=True)
    down_full = lax.all_gather(w_down, "row", axis=1, tiled=True)
    gain_one_full = lax.all_gather(gain_one, "row", axis=0, tiled=True)
    gain_two_full = lax.all_gather(gain_two, "row", axis=0, tiled=True)

    both = lax.all_to_all(
        jnp.stack([layer_in, cotangent]), "row", split_axis=1, concat_axis=2, tiled=True
    )
    x_own = both[0].astype(F32)
    cot_own = both[1]
    full_width = x_own.shape[1]

    def norm_forward(rows, gain):
        inverse = lax.rsqrt(jnp.mean(rows * rows, axis=1, keepdims=True) + EPS)
        return inverse, (rows * inverse * gain).astype(BF)

    def norm_back(grad_normed, rows, inverse, gain):
        weighted = grad_normed * gain
        mean = jnp.mean(weighted * rows, axis=1, keepdims=True)
        grad_rows = inverse * weighted - rows * inverse**3 * mean
        return grad_rows, jnp.sum(grad_normed * rows * inverse, axis=0)

    inverse_one, normed_one = norm_forward(x_own, gain_one_full)
    normed_full = token_gather(normed_one)
    cot_full = token_gather(cot_own)

    bias = jnp.concatenate(
        [
            b_query,
            lax.dynamic_slice_in_dim(b_key, shared_head * HD, HD, 0),
            lax.dynamic_slice_in_dim(b_value, shared_head * HD, HD, 0),
        ]
    )
    qkv = matmul(normed_full, w_qkv) + bias
    query_rot = rotary(
        qkv[:, :head_width].reshape(query_count, heads_here, HD), cosine, sine
    ).astype(BF)
    key_own = rotary(qkv[:, head_width : head_width + HD][:, None, :], cosine, sine)[:, 0]
    kv_own = jnp.concatenate([key_own, qkv[:, head_width + HD :]], axis=1).astype(BF)
    kv_all = lax.all_gather(kv_own, "row", axis=0, tiled=True)
    key_rot, value_low = kv_all[:, :HD], kv_all[:, HD:]

    def score_of():
        scores = jnp.einsum("qhd,kd->hqk", query_rot, key_rot, preferred_element_type=F32)
        return jnp.where(allowed[None], scores * score_scale, MASKED)

    scores = score_of()
    row_peak = jnp.max(scores, axis=-1, keepdims=True)
    exponent = jnp.exp(scores - row_peak)
    row_total = jnp.sum(exponent, axis=-1, keepdims=True)
    weights = (exponent / row_total).astype(BF)
    heads_out = (
        jnp.einsum("hqk,kd->qhd", weights, value_low, preferred_element_type=F32)
        .reshape(query_count, head_width)
        .astype(BF)
    )
    log_total = row_peak + jnp.log(row_total)

    hidden_state = x_own + token_reduce(matmul(heads_out, wo_full))
    inverse_two, normed_two = norm_forward(hidden_state, gain_two_full)
    normed_two_full = token_gather(normed_two)

    gate_pre = matmul(normed_two_full, gate_full)
    up_pre = matmul(normed_two_full, up_full)
    gate_sigmoid = jax.nn.sigmoid(gate_pre)
    silu_gate = gate_pre * gate_sigmoid
    inner = (silu_gate * up_pre).astype(BF)
    layer_own = (hidden_state + token_reduce(matmul(inner, down_full))).astype(BF)

    block_order = (1, 3, 0, 2)

    def by_block(values):
        return jnp.concatenate(
            [
                lax.dynamic_slice_in_dim(values, (row_place ^ step) * width, width, 1)
                for step in block_order
            ],
            axis=1,
        )

    cot_blocks = by_block(cot_full)
    normed_two_blocks = by_block(normed_two_full)
    normed_one_blocks = by_block(normed_full)

    def pair(blocks, which):
        return blocks[:, : 2 * width] if which else blocks[:, 2 * width :]

    grad_w_down = weight_total(lambda which: contract_rows(inner, pair(cot_blocks, which)), 1)
    grad_inner = contract_cols(cot_full, down_full)
    grad_gate = (
        grad_inner * up_pre * gate_sigmoid * (1.0 + gate_pre * (1.0 - gate_sigmoid))
    ).astype(BF)
    grad_up = (grad_inner * silu_gate).astype(BF)
    grad_normed_two = token_reduce(
        contract_cols(grad_gate, gate_full) + contract_cols(grad_up, up_full)
    )
    grad_w_gate = weight_total(
        lambda which: contract_rows(pair(normed_two_blocks, which), grad_gate), 0
    )
    grad_w_up = weight_total(
        lambda which: contract_rows(pair(normed_two_blocks, which), grad_up), 0
    )
    grad_hidden_norm, grad_gain_two = norm_back(
        grad_normed_two, hidden_state, inverse_two, gain_two_full
    )
    grad_hidden = cot_own.astype(F32) + grad_hidden_norm
    grad_attn = token_gather(grad_hidden.astype(BF))
    grad_attn_blocks = by_block(grad_attn)
    grad_w_out = weight_total(
        lambda which: contract_rows(heads_out, pair(grad_attn_blocks, which)), 1
    )
    grad_heads = (
        contract_cols(grad_attn, wo_full).astype(BF).reshape(query_count, heads_here, HD)
    )

    scores = score_of()
    weights = jnp.exp(scores - log_total)
    grad_weights = jnp.einsum("qhd,kd->hqk", grad_heads, value_low, preferred_element_type=F32)
    inner_sum = jnp.sum(weights * grad_weights, axis=-1, keepdims=True)
    grad_scores = (weights * (grad_weights - inner_sum)).astype(BF)
    weights_low = weights.astype(BF)
    grad_query_rot = (
        jnp.einsum("hqk,kd->qhd", grad_scores, key_rot, preferred_element_type=F32) * score_scale
    )
    key_total = (
        jnp.einsum("hqk,qhd->kd", grad_scores, query_rot, preferred_element_type=F32) * score_scale
    )
    value_total = jnp.einsum("hqk,qhd->kd", weights_low, grad_heads, preferred_element_type=F32)
    grad_query = rotary_back(grad_query_rot, cosine, sine).reshape(query_count, head_width)
    kv_sums = lax.psum_scatter(
        jnp.concatenate([key_total, value_total], axis=1).astype(BF),
        "row",
        scatter_dimension=0,
        tiled=True,
    ).astype(F32)
    grad_key = rotary_back(kv_sums[:, None, :HD], cosine, sine)[:, 0]
    grad_qkv = jnp.concatenate([grad_query, grad_key, kv_sums[:, HD:]], axis=1).astype(BF)
    grad_normed_one = token_reduce(contract_cols(grad_qkv, w_qkv))
    grad_w_qkv = weight_total(
        lambda which: contract_rows(pair(normed_one_blocks, which), grad_qkv), 0
    )
    grad_b_qkv = jnp.sum(grad_qkv, axis=0, dtype=F32)
    grad_state_norm, grad_gain_one = norm_back(grad_normed_one, x_own, inverse_one, gain_one_full)
    grad_in_own = grad_hidden + grad_state_norm

    layer_out = lax.all_to_all(layer_own, "row", split_axis=1, concat_axis=0, tiled=True)
    grad_input = lax.all_to_all(
        grad_in_own.astype(BF), "row", split_axis=1, concat_axis=0, tiled=True
    ).astype(F32)

    w_qkv_total = pack_total(grad_w_qkv)
    kv_parts = lax.all_gather(w_qkv_total[:, head_width:].astype(BF), "col", axis=0).astype(F32)
    cols_each = col_devices // KV
    kv_heads = kv_parts.reshape(KV, cols_each, width, 2, HD).sum(axis=1)
    grad_w_key = kv_heads[:, :, 0].transpose(1, 0, 2).reshape(width, KV * HD)
    grad_w_value = kv_heads[:, :, 1].transpose(1, 0, 2).reshape(width, KV * HD)

    slots = jnp.zeros((2, KV * HD), F32)
    slots = lax.dynamic_update_slice(
        slots, grad_b_qkv[head_width:].reshape(2, HD), (0, shared_head * HD)
    )
    query_slots = lax.dynamic_update_slice(
        jnp.zeros((HEADS * HD,), F32), grad_b_qkv[:head_width], (col_place * head_width,)
    )
    small = jnp.concatenate([grad_gain_one, grad_gain_two, query_slots, slots.reshape(-1)])
    small = lax.psum(small, ("dp", "row", "col"))
    own_cols = row_place * width
    return (
        layer_out,
        grad_input,
        lax.dynamic_slice_in_dim(small, own_cols, width, 0),
        w_qkv_total[:, :head_width],
        lax.dynamic_slice_in_dim(small, 2 * full_width + col_place * head_width, head_width, 0),
        grad_w_key,
        small[2 * full_width + HEADS * HD :][: KV * HD],
        grad_w_value,
        small[2 * full_width + HEADS * HD + KV * HD :],
        pack_total(grad_w_out),
        lax.dynamic_slice_in_dim(small, full_width + own_cols, width, 0),
        pack_total(grad_w_gate),
        pack_total(grad_w_up),
        pack_total(grad_w_down),
    )


def solution(mesh):
    return jax.shard_map(
        body,
        mesh=mesh,
        in_specs=(
            P(("dp", "col"), "row"),
            P(("dp", "col"), "row"),
            P("dp", None),
            P("dp", None),
            P("row"),
            P("row", "col"),
            P("col"),
            P("row", None),
            P(),
            P("row", None),
            P(),
            P("col", "row"),
            P("row"),
            P("row", "col"),
            P("row", "col"),
            P("col", "row"),
        ),
        out_specs=(
            P(("dp", "col"), "row"),
            P(("dp", "col"), "row"),
            P("row"),
            P("row", "col"),
            P("col"),
            P("row", None),
            P(),
            P("row", None),
            P(),
            P("col", "row"),
            P("row"),
            P("row", "col"),
            P("row", "col"),
            P("col", "row"),
        ),
        check_vma=False,
    )
```
